32 devices in a mesh: blk: 16 (over z, y, core), head: 2 (over x).
Axes of the slice: x: 2, y: 2, z: 4, core: 2. Of those that a mesh axis runs over, the one named last changes fastest.
Arguments:
- query_nope: bfloat16 [1024, 8192], P('blk', 'head'), may hold values from -140 to 140
- query_rope: bfloat16 [1024, 4096], P('blk', 'head'), may hold values from -6 to 6
- compressed: bfloat16 [1024, 576], P(('blk', 'head')), may hold values from -6 to 6
- latent_gain: float32 [512], replicated, may hold values from 0.1 to 1.9
- key_up: bfloat16 [64, 128, 512], P('head'), may hold values from -0.5 to 0.5
- value_up: bfloat16 [64, 512, 128], P('head'), may hold values from -1.5 to 1.5
- span_order: int32 [32], replicated, may hold values from 0 to 31, each once
Outputs:
- attended: bfloat16 [1024, 8192], P('blk', 'head')
The draws below stay inside these ranges and needn't reach their ends.
Inputs may be any that keep to these rules, and one draw needn't show every extreme that they name: Every number appears once; device index i of blk holds the blocks span_order[2 i] and span_order[2 i + 1].
All inputs are finite; a program needn't handle non-finite values.
Results may differ from the reference program's by a relative error of at most 0.0075.
The reference program's roundings to bfloat16 on the way count: a program that leaves them out, or rounds other values in their place, can miss the bound.
Values may be sent and summed in bfloat16 or wider, within the bound.
A program may use at most 64 MiB of HBM per device.

```python
import jax
import jax.numpy as jnp
from jax import lax

LATENT = 512
ROPE = 64
NOPE = 128
VDIM = 128
HEADS = 64
TOK_DEV = 64
TOKENS = 1024
N_BLK = 16


def draw_query_nope(key, part):
    first_key = jax.random.fold_in(jax.random.fold_in(key, 17), 0)
    values = jax.random.truncated_normal(first_key, -6.0, 6.0, (TOKENS, HEADS, NOPE), jnp.float32)
    return values.reshape(TOKENS, HEADS * NOPE).astype(jnp.bfloat16)


def block_levels(rng, dims, cuts, low, high):
    def one(position, blocks):
        steps = jax.random.uniform(jax.random.fold_in(jax.random.fold_in(rng, 6), position), (blocks,), jnp.float32, low / len(cuts), high / len(cuts))
        return jnp.repeat(jnp.exp(steps), dims[position] // blocks).reshape((-1,) + (1,) * (len(dims) - position - 1))

    loudness = one(*cuts[0])
    for cut in cuts[1:]:
        loudness = loudness * one(*cut)
    return loudness


def normal_values(own_key, shape, width, limit, cuts=(), kind=jnp.bfloat16):
    factor_of = block_levels(own_key, shape, cuts, -0.22, 0.18) if cuts else 1.0
    drawn = jax.random.normal(own_key, shape, jnp.float32) * width * factor_of
    return jnp.minimum(jnp.maximum(drawn, -limit), limit).astype(kind)


def setup_inputs(seed: int = 0) -> dict:
    arg_keys = jax.random.split(jax.random.key(seed), 8)
    return {
        "query_nope": draw_query_nope(jax.random.fold_in(arg_keys[7], 71), 0),
        "query_rope": normal_values(arg_keys[1], (TOKENS, HEADS * ROPE), 1.0, 6.0, ((0, 16), (1, 2))),
        "compressed": normal_values(arg_keys[2], (TOKENS, LATENT + ROPE), 1.0, 6.0, ((0, 32),)),
        "latent_gain": jnp.clip(1.0 + 0.18 * jax.random.normal(arg_keys[3], (LATENT,), jnp.float32), 0.1, 1.9),
        "key_up": normal_values(arg_keys[4], (HEADS, NOPE, LATENT), NOPE ** -0.5, 0.5, ((0, 2),)),
        "value_up": normal_values(arg_keys[5], (HEADS, LATENT, VDIM), (LATENT // 32) ** -0.5, 1.5, ((0, 2),)),
        "span_order": jax.random.permutation(arg_keys[6], 2 * N_BLK).astype(jnp.int32),
    }


norm_epsilon = 1e-06
rope_base = 10000.0
masked_score = -1e+30

def lookup(entries, index_array):
    slots = jnp.arange(entries.shape[0], dtype=jnp.int32)
    matches = index_array[..., None] == slots
    return lax.optimization_barrier(jnp.sum(jnp.where(matches, entries, 0), axis=-1)).astype(jnp.int32)

def rotate(values, positions):
    half_width = values.shape[-1] // 2
    frequency = rope_base ** (-jnp.arange(half_width, dtype=jnp.float32) / half_width)
    angles = positions.astype(jnp.float32)[..., None] * frequency
    cosine = jnp.cos(angles)
    sine_value = jnp.sin(angles)
    leading = values[..., :half_width]
    trailing = values[..., half_width:]
    return jnp.concatenate([leading * cosine - trailing * sine_value, leading * sine_value + trailing * cosine], axis=-1)

def reference(query_nope, query_rope, compressed, latent_gain, key_up, value_up, span_order):
    half_block = TOK_DEV // 2
    row_ids = jnp.arange(TOKENS, dtype=jnp.int32)
    positions = lookup(span_order, row_ids // half_block) * half_block + row_ids % half_block
    latent = compressed[:, :LATENT].astype(jnp.float32)
    latent = latent * lax.rsqrt(lax.optimization_barrier(jnp.mean(latent * latent, axis=1, keepdims=True)) + norm_epsilon) * latent_gain
    latent = latent.astype(jnp.bfloat16)
    key_rot = rotate(compressed[:, LATENT:].astype(jnp.float32), positions).astype(jnp.bfloat16)
    key_matrix = jnp.concatenate([latent, key_rot], axis=1)
    nope_parts = query_nope.reshape(TOKENS, HEADS, NOPE)
    query_rot = rotate(query_rope.reshape(TOKENS, HEADS, ROPE).astype(jnp.float32), positions[:, None]).astype(jnp.bfloat16)
    visible = positions[None, :] <= positions[:, None]
    score_scale = (NOPE + ROPE) ** (-0.5)

    def one_head(head_index):
        query_lat = jnp.dot(nope_parts[:, head_index, :], key_up[head_index], preferred_element_type=jnp.float32).astype(jnp.bfloat16)
        queries = jnp.concatenate([query_lat, query_rot[:, head_index, :]], axis=1)
        scores = jnp.dot(queries, key_matrix.T, preferred_element_type=jnp.float32) * score_scale
        scores = jnp.where(visible, scores, masked_score)
        row_max = lax.optimization_barrier(jnp.max(scores, axis=1, keepdims=True))
        weight = jnp.where(visible, jnp.exp(scores - row_max), 0.0)
        totals = lax.optimization_barrier(jnp.sum(weight, axis=1, keepdims=True))
        lat_out = jnp.dot(weight.astype(jnp.bfloat16), latent, preferred_element_type=jnp.float32) / totals
        lat_out = lat_out.astype(jnp.bfloat16)
        return jnp.dot(lat_out, value_up[head_index], preferred_element_type=jnp.float32).astype(jnp.bfloat16)
    outputs = lax.map(one_head, jnp.arange(HEADS, dtype=jnp.int32))
    return jnp.transpose(outputs, (1, 0, 2)).reshape(TOKENS, HEADS * VDIM)
```

```python
import functools
import math

import jax
import jax.numpy as jnp
import numpy as np
from jax import lax
from jax.experimental import pallas as pl
from jax.experimental.pallas import tpu as pltpu
from jax.sharding import PartitionSpec as P

norm_epsilon = 1e-06
rope_base = 10000.0
masked_score = -1e30
LANES = 128
GROUP = 8
MESH = pl.DeviceIdType.MESH


def rotate_tile(tile, cosine, signed_sine, rope_width):
    half = rope_width // 2
    width = tile.shape[-1]
    lane = lax.broadcasted_iota(jnp.int32, tile.shape, 1)
    partner = jnp.where(
        lane % rope_width < half,
        pltpu.roll(tile, width - half, 1),
        pltpu.roll(tile, half, 1),
    )
    return tile * cosine + partner * signed_sine


def angles_of(positions, freq, rope_width):
    angles = positions.astype(jnp.float32) * freq
    lane = lax.broadcasted_iota(jnp.int32, angles.shape, 1)
    sine = jnp.sin(angles)
    return jnp.cos(angles), jnp.where(lane % rope_width < rope_width // 2, -sine, sine)


def body(
    dims,
    remote,
    span_ref,
    keys_in_ref,
    gain_ref,
    freq_ref,
    nope_hbm,
    rope_hbm,
    key_up_hbm,
    value_up_hbm,
    out_hbm,
    nope_ref,
    rope_ref,
    key_up_ref,
    value_up_ref,
    out_ref,
    keys_ref,
    query_ref,
    mask_ref,
    load_sem,
    out_sem,
    send_sem,
    recv_sem,
):
    tokens, heads, nope, latent, rope, value, total, slices = dims
    half_block = tokens // 2
    scale = (nope + rope) ** (-0.5) * math.log2(math.e)
    blk = lax.axis_index("blk")
    head = lax.axis_index("head")
    loads = [
        pltpu.make_async_copy(nope_hbm, nope_ref, load_sem.at[0]),
        pltpu.make_async_copy(rope_hbm, rope_ref, load_sem.at[1]),
        pltpu.make_async_copy(key_up_hbm, key_up_ref, load_sem.at[2]),
        pltpu.make_async_copy(value_up_hbm, value_up_ref, load_sem.at[3]),
    ]
    for load in loads:
        load.start()

    sends = []
    if remote:
        outer = lax.axis_size("blk") // 4
        o, i, c = blk // 4, (blk // 2) % 2, blk % 2

        def device(o_, i_, c_, h_):
            return ((o_ * 2 + i_) * 2 + c_, h_)

        def slot(o_, i_, c_, h_):
            return ((o_ * 2 + i_) * 2 + c_) * 2 + h_

        def block_at(index):
            return keys_ref.at[pl.ds(pl.multiple_of(index * slices, slices), slices)]

        def send(index, target):
            copy = pltpu.make_async_remote_copy(
                src_ref=block_at(index),
                dst_ref=block_at(index),
                send_sem=send_sem.at[len(sends)],
                recv_sem=recv_sem.at[index],
                device_id=target,
                device_id_type=MESH,
            )
            copy.start()
            sends.append(copy)

        def arrive(index):
            pltpu.make_async_remote_copy(
                src_ref=block_at(index),
                dst_ref=block_at(index),
                send_sem=send_sem.at[0],
                recv_sem=recv_sem.at[index],
                device_id=device(o, i, 1 - c, head),
                device_id_type=MESH,
            ).wait_recv()

        sibling = device(o, i, 1 - c, head)
        i_peer = device(o, 1 - i, c, head)
        h_peer = device(o, i, c, 1 - head)
        order = []
        for d in range(1, outer // 2 + 1):
            order.append(d)
            if d != outer - d:
                order.append(outer - d)
        at = lambda d: lax.rem(o + d, outer)
        o_peers = [device(at(d), i, c, head) for d in order]
        peers = [sibling, i_peer, h_peer] + o_peers
        barrier = pltpu.get_barrier_semaphore()
        for peer in peers:
            pl.semaphore_signal(barrier, inc=1, device_id=peer, device_id_type=MESH)

        first_row = blk * tokens + head * slices
        own_pos = (
            span_ref[first_row // half_block] * half_block
            + first_row % half_block
            + lax.broadcasted_iota(jnp.int32, (slices, LANES), 0)
        )
        own = keys_in_ref[...].astype(jnp.float32)
        own_latent = own[:, :latent]
        own_latent = (
            own_latent
            * lax.rsqrt(jnp.mean(own_latent * own_latent, axis=1, keepdims=True) + norm_epsilon)
            * gain_ref[...]
        )
        cosine, sine = angles_of(own_pos, freq_ref[...], rope)
        own_rope = own[:, latent : latent + rope]
        own_rope = jnp.concatenate([own_rope] * (LANES // rope), axis=1)
        own_slot = slot(o, i, c, head)
        own_block = block_at(own_slot)
        own_block[:, :latent] = own_latent.astype(jnp.bfloat16)
        own_block[:, latent:] = rotate_tile(own_rope, cosine, sine, rope).astype(jnp.bfloat16)

        pl.semaphore_wait(barrier, len(peers))
        for peer in [i_peer, h_peer] + o_peers + [sibling]:
            send(own_slot, peer)
    else:
        keys_copy = pltpu.make_async_copy(keys_in_ref, keys_ref, load_sem.at[4])
        keys_copy.start()

    token = lax.broadcasted_iota(jnp.int32, (tokens, LANES), 0)
    query_pos = (
        jnp.where(token < half_block, span_ref[blk * 2], span_ref[blk * 2 + 1]) * half_block
        + token % half_block
    )
    key_lane = lax.broadcasted_iota(jnp.int32, (8, total), 1)
    key_half = key_lane // half_block
    key_span = jnp.zeros((8, total), jnp.int32)
    for entry in range(total // half_block):
        key_span = jnp.where(key_half == entry, span_ref[entry], key_span)
    key_pos = key_span * half_block + key_lane % half_block
    mask_ref[...] = jnp.where(key_pos[:1] <= query_pos[:, :1], 0.0, masked_score)
    cosine, sine = angles_of(query_pos, freq_ref[...], rope)
    loads[1].wait()
    per_tile = LANES // rope
    lane = lax.broadcasted_iota(jnp.int32, (tokens, LANES), 1)
    for tile in range(heads // per_tile):
        columns = rope_ref[:, tile * LANES : (tile + 1) * LANES].astype(jnp.float32)
        rotated = rotate_tile(columns, cosine, sine, rope)
        for part in range(per_tile):
            row = (tile * per_tile + part) * tokens
            query_ref[row : row + tokens, latent:] = jnp.where(
                lane // rope == part, rotated, 0.0
            ).astype(jnp.bfloat16)

    if remote:
        for d in order:
            index = slot(at(d), i, c, head)
            arrive(index)
            for peer in (i_peer, h_peer, sibling):
                send(index, peer)

    loads[0].wait()
    loads[2].wait()

    def lift(first, count):
        for h in range(first, first + count):
            query_ref[h * tokens : (h + 1) * tokens, :latent] = jnp.dot(
                nope_ref[:, h * nope : (h + 1) * nope],
                key_up_ref[h],
                preferred_element_type=jnp.float32,
            ).astype(jnp.bfloat16)

    if remote:
        steps = [0] + order
        per_step = -(-heads // len(steps))
        for n, d in enumerate(steps):
            lift(n * per_step, max(0, min(per_step, heads - n * per_step)))
            via_h, via_i = slot(at(d), i, c, 1 - head), slot(at(d), 1 - i, c, head)
            arrive(via_i)
            if d % 2 == 1:
                send(via_i, h_peer)
            send(via_i, sibling)
            arrive(via_h)
            if d % 2 == 0:
                send(via_h, i_peer)
            send(via_h, sibling)
        for d in steps:
            index = slot(at(d), 1 - i, c, 1 - head)
            arrive(index)
            send(index, sibling)
        for d in steps:
            for i_ in (i, 1 - i):
                for h_ in (head, 1 - head):
                    arrive(slot(at(d), i_, 1 - c, h_))
    else:
        lift(0, heads)
        keys_copy.wait()
    loads[3].wait()

    group = min(GROUP, heads)
    rows = group * tokens

    def attend(g, _):
        start = pl.multiple_of(g * rows, rows)
        scores = lax.dot_general(
            query_ref[pl.ds(start, rows), :],
            keys_ref[...],
            (((1,), (1,)), ((), ())),
            preferred_element_type=jnp.float32,
        )
        scores = scores.reshape(group, tokens, total) + mask_ref[...][None]
        top = jnp.max(scores, axis=2, keepdims=True)
        weight = jnp.exp2((scores - top) * scale)
        sums = jnp.sum(weight, axis=2, keepdims=True).reshape(rows, 1)
        product = jnp.dot(
            weight.reshape(rows, total).astype(jnp.bfloat16),
            keys_ref[:, :latent],
            preferred_element_type=jnp.float32,
        )
        lat_out = (product * (1.0 / sums)).astype(jnp.bfloat16)
        for n in range(group):
            column = pl.multiple_of((g * group + n) * value, value)
            out_ref[:, pl.ds(column, value)] = jnp.dot(
                lat_out[n * tokens : (n + 1) * tokens],
                value_up_ref[g * group + n],
                preferred_element_type=jnp.float32,
            ).astype(jnp.bfloat16)
        return 0

    lax.fori_loop(0, heads // group, attend, 0)
    store = pltpu.make_async_copy(out_ref, out_hbm, out_sem.at[0])
    store.start()
    for copy in sends:
        copy.wait_send()
    store.wait()


def shards(
    mesh, query_nope, query_rope, compressed, latent_gain, key_up, value_up, span_order
):
    tokens, (heads, nope, latent) = query_nope.shape[0], key_up.shape
    rope, value = query_rope.shape[1] // heads, value_up.shape[2]
    slices = compressed.shape[0]
    blocks, head_parts = mesh.shape["blk"], mesh.shape["head"]
    total = blocks * tokens
    half_block = tokens // 2
    half = rope // 2
    remote = head_parts == 2 and blocks % 4 == 0 and slices % 16 == 0 and half_block % slices == 0
    exponents = np.arange(LANES) % half
    freq = jnp.asarray((rope_base ** (-exponents / half)).astype(np.float32))[None]
    gain = latent_gain[None]
    if remote:
        keys_in = compressed
    else:
        rows = (
            lax.axis_index("blk") * tokens
            + lax.axis_index("head") * slices
            + jnp.arange(slices, dtype=jnp.int32)
        )
        pos = span_order[rows // half_block] * half_block + rows % half_block
        wide = compressed.astype(jnp.float32)
        lat = wide[:, :latent]
        lat = lat * lax.rsqrt(jnp.mean(lat * lat, axis=1, keepdims=True) + norm_epsilon) * gain
        angles = pos.astype(jnp.float32)[:, None] * freq[:, :half]
        a, b = wide[:, latent : latent + half], wide[:, latent + half :]
        cosine, sine = jnp.cos(angles), jnp.sin(angles)
        rot = [a * cosine - b * sine, a * sine + b * cosine]
        own = jnp.concatenate([lat] + rot * (LANES // rope), axis=1).astype(jnp.bfloat16)
        keys_in = lax.all_gather(own, ("blk", "head"), axis=0, tiled=True)
    any_space = pl.BlockSpec(memory_space=pl.ANY)
    vmem = pl.BlockSpec(memory_space=pltpu.VMEM)
    dims = (tokens, heads, nope, latent, rope, value, total, slices)
    return pl.pallas_call(
        functools.partial(body, dims, remote),
        out_shape=jax.ShapeDtypeStruct((tokens, heads * value), jnp.bfloat16),
        in_specs=[
            pl.BlockSpec(memory_space=pltpu.SMEM),
            vmem if remote else any_space,
            vmem,
            vmem,
            any_space,
            any_space,
            any_space,
            any_space,
        ],
        out_specs=any_space,
        scratch_shapes=[
            pltpu.VMEM(query_nope.shape, jnp.bfloat16),
            pltpu.VMEM(query_rope.shape, jnp.bfloat16),
            pltpu.VMEM(key_up.shape, jnp.bfloat16),
            pltpu.VMEM(value_up.shape, jnp.bfloat16),
            pltpu.VMEM((tokens, heads * value), jnp.bfloat16),
            pltpu.VMEM((total, latent + LANES), jnp.bfloat16),
            pltpu.VMEM((heads * tokens, latent + LANES), jnp.bfloat16),
            pltpu.VMEM((tokens, total), jnp.float32),
            pltpu.SemaphoreType.DMA((5,)),
            pltpu.SemaphoreType.DMA((1,)),
            pltpu.SemaphoreType.DMA((2 * blocks if remote else 1,)),
            pltpu.SemaphoreType.DMA((2 * blocks if remote else 1,)),
        ],
        compiler_params=pltpu.CompilerParams(
            vmem_limit_bytes=60 * 1024 * 1024,
            has_side_effects=remote,
            **({"collective_id": 0} if remote else {}),
        ),
    )(span_order, keys_in, gain, freq, query_nope, query_rope, key_up, value_up)


def solution(mesh):
    in_specs = (
        P("blk", "head"),
        P("blk", "head"),
        P(("blk", "head"), None),
        P(),
        P("head", None, None),
        P("head", None, None),
        P(),
    )
    return jax.shard_map(
        functools.partial(shards, mesh),
        mesh=mesh,
        in_specs=in_specs,
        out_specs=P("blk", "head"),
        check_vma=False,
    )
```
